32 devices in a mesh: dp: 16 (over z, y, core), tensor: 2 (over x).
Axes of the slice: x: 2, y: 2, z: 4, core: 2. Of those that a mesh axis runs over, the one named last changes fastest.
Arguments:
- expert_act: bfloat16 [16384, 2880], P(('dp', 'tensor')), may hold values from -6 to 6
- grad_out: bfloat16 [32768, 1440], P(('dp', 'tensor')), may hold values from -6 to 6
- slot_token: int32 [16384], P(('dp', 'tensor')), may hold values from 0 to 1023, as said below
- slot_prob: float32 [16384], P(('dp', 'tensor')), may hold values from 0.2 to 1
- live_count: int32 [32], P(('dp', 'tensor')), may hold values from 128 to 512, as said below
Outputs:
- weight_grad: float32 [2880, 1440], P('dp', 'tensor')
The draws below stay inside these ranges and needn't reach their ends.
Inputs may be any that keep to these rules, and one draw needn't show every extreme that they name: `slot_token`: each device's 512 entries are distinct token indices of that device. `live_count`: each entry is 512 // j for some j of 1 to 4.
All inputs are finite; a program needn't handle non-finite values.
Results may differ from the reference program's by a relative error of at most 0.0029.
Values may be sent and summed in bfloat16 or wider, within the bound.
A program may use at most 128 MiB of HBM per device.

```python
import math
import jax
import jax.numpy as jnp
from jax import lax

D = 1440
FF = 2880
CAP = 512
TOK_DEV = 1024
SLOTS = 16384
TOKENS = 32768


def draw_slot_token(key, part):
    device_total = SLOTS // CAP
    device_keys = jax.random.split(jax.random.fold_in(key, 11), device_total)

    def shuffled(seed_key):
        return jax.random.permutation(seed_key, TOK_DEV)[:CAP].astype(jnp.int32)
    return jax.vmap(shuffled)(device_keys).reshape(-1).astype(jnp.int32)


def draw_live_count(key, part):
    device_total = SLOTS // CAP
    first_key = jax.random.fold_in(key, 21)
    second_key = jax.random.fold_in(key, 22)
    divisor = jax.random.randint(first_key, (device_total,), 1, 5)
    counted = (CAP // divisor).astype(jnp.int32)
    fullest = jax.random.randint(second_key, (), 0, device_total)
    return counted.at[fullest].set(CAP).astype(jnp.int32)


def block_levels(key, shape, shards, low, high):
    factor_of = 1.0
    for dim, blocks in shards:
        steps = jax.random.uniform(jax.random.fold_in(jax.random.fold_in(key, 6), dim), (blocks,), jnp.float32, low / len(shards), high / len(shards))
        factor_of = factor_of * jnp.repeat(jnp.exp(steps), shape[dim] // blocks).reshape((-1,) + (1,) * (len(shape) - 1 - dim))
    return factor_of


def normal_values(stream_key, dims, width, reach, pieces=(), kind=jnp.bfloat16):
    entries = jax.random.normal(stream_key, dims, jnp.float32) * width
    if len(pieces) > 0:
        entries = block_levels(stream_key, dims, pieces, -0.22, 0.18) * entries
    return jnp.clip(entries, min=-reach, max=reach).astype(kind)


def setup_inputs(seed: int = 0) -> dict:
    splits = jax.random.split(jax.random.key(seed), 6)
    expert_act = normal_values(splits[0], (SLOTS, FF), 1.0, 6.0, ((0, 32),))
    grad_out = normal_values(splits[1], (TOKENS, D), 1.0, 6.0, ((0, 32),))
    slot_token = draw_slot_token(jax.random.fold_in(splits[5], 71), 0)
    slot_prob = jnp.clip(jnp.exp(math.log(1.0) - 1.609438 * jax.random.uniform(splits[3], (SLOTS,), jnp.float32) ** block_levels(splits[3], (SLOTS,), ((0, 32),), -0.2, 0.2)), 0.2, 1.0)
    live_count = draw_live_count(jax.random.fold_in(splits[5], 71), 0)
    return dict(expert_act=expert_act, grad_out=grad_out, slot_token=slot_token, slot_prob=slot_prob, live_count=live_count)


def reference(expert_act, grad_out, slot_token, slot_prob, live_count):
    slot_total = expert_act.shape[0]
    position = jnp.arange(slot_total, dtype=jnp.int32)
    owner_dev = (position // CAP).astype(jnp.int32)
    token_rows = (slot_token + owner_dev * TOK_DEV).astype(jnp.int32)
    live_mask = position % CAP < live_count[owner_dev]
    weighting = jnp.where(live_mask, slot_prob, jnp.zeros_like(slot_prob))
    picked = grad_out[token_rows].astype(jnp.float32)
    weighted = (picked * weighting[:, None]).astype(jnp.bfloat16)
    gradient = lax.dot_general(expert_act, weighted, (((0,), (0,)), ((), ())), preferred_element_type=jnp.float32)
    return gradient * (1.0 / math.sqrt(slot_total))
```

```python
import functools
import math

import jax
import jax.numpy as jnp
from jax import lax
from jax.experimental import pallas as pl
from jax.experimental.pallas import tpu as pltpu
from jax.sharding import PartitionSpec as P

MESH = pl.DeviceIdType.MESH
LANES = 128


def kernel(
    outer, wide,
    acts_hbm, grad_hbm, token_hbm, prob_hbm, live_ref, out_ref,
    token_ref, prob_ref, acts_raw, grad_raw, rest_raw, acts, peer_acts,
    mine, peer, mine_rest, peer_rest,
    send_a, recv_a, send_b, recv_b, send_z, recv_z,
    send_r, recv_r, own_r, send_p, recv_p, turned,
    small_sems, load_sems, grad_sems, acts_sems, w_sems,
    a_sems, b_sems, z_sems, r_sems, p_sems,
):
    dp = lax.axis_index("dp")
    half = lax.axis_index("tensor")
    core = lax.rem(dp, 2)
    mid = lax.rem(dp // 2, 2)
    own = dp // 4
    my_a = half * (1 - core) + mid * core
    my_b = mid * (1 - core) + half * core
    flip_mid = dp + 2 - 4 * mid
    pair_dev = {"dp": dp + 1 - 2 * core, "tensor": half}
    x_dev = {"dp": dp, "tensor": 1 - half}
    y_dev = {"dp": flip_mid, "tensor": half}
    xy_dev = {"dp": flip_mid, "tensor": 1 - half}
    a_dev = {
        "dp": dp * (1 - core) + flip_mid * core,
        "tensor": (1 - half) * (1 - core) + half * core,
    }
    b_dev = {
        "dp": flip_mid * (1 - core) + dp * core,
        "tensor": half * (1 - core) + (1 - half) * core,
    }
    last = outer - 1
    rows = acts.shape[3]
    rest = rest_raw.shape[0] // 2

    def target(step):
        offset = outer // 2 + step // 2 - (step % 2) * step
        return lax.rem(own + offset, outer)

    def z_dev(step):
        return {"dp": dp + (target(step) - own) * 4, "tensor": half}

    def remote(src, dst, send, recv, device):
        return pltpu.make_async_remote_copy(
            src_ref=src, dst_ref=dst, send_sem=send, recv_sem=recv,
            device_id=device, device_id_type=MESH,
        )

    grad_order = (1 - half, half)
    load_small = [
        pltpu.make_async_copy(token_hbm, token_ref, small_sems.at[0]),
        pltpu.make_async_copy(prob_hbm, prob_ref, small_sems.at[1]),
    ]
    load_wide = [
        pltpu.make_async_copy(
            grad_hbm.at[g, pl.ds(0, wide)], grad_raw.at[g], grad_sems.at[i]
        )
        for i, g in enumerate(grad_order)
    ]
    load_rest = [
        pltpu.make_async_copy(
            grad_hbm.at[g, pl.ds(wide, rest)], rest_raw.at[pl.ds(g * rest, rest)],
            grad_sems.at[2 + g],
        )
        for g in range(2)
    ]

    def load_acts(step):
        o = target(step)
        return pltpu.make_async_copy(acts_hbm.at[o], acts_raw.at[o], load_sems.at[step])

    for copy in load_small:
        copy.start()
    load_wide[0].start()
    load_acts(0).start()
    for copy in load_rest:
        copy.start()
    load_wide[1].start()

    barrier = pltpu.get_barrier_semaphore()
    for device in [pair_dev, x_dev, y_dev, xy_dev] + [z_dev(s) for s in range(last)]:
        pl.semaphore_signal(barrier, inc=1, device_id=device, device_id_type=MESH)

    def start_acts(step, carry):
        load_acts(step).start()
        return carry

    lax.fori_loop(1, outer, start_acts, 0)

    slots, tokens = token_ref.shape[1], grad_raw.shape[2]
    load_small[0].wait()
    load_small[1].wait()
    chosen = lax.broadcasted_iota(jnp.int32, (tokens, slots), 0) == token_ref[...]
    onehot = jnp.where(chosen, 1.0, 0.0).astype(jnp.bfloat16)
    live = lax.broadcasted_iota(jnp.int32, (1, slots), 1) < live_ref[0]
    weight = jnp.where(live, prob_ref[...], 0.0)

    def weigh(raw):
        picked = jnp.dot(raw, onehot, preferred_element_type=jnp.float32)
        return (picked * weight).astype(jnp.bfloat16)

    def copy_wide(i):
        g = grad_order[i]
        return remote(mine.at[g], peer.at[g], w_sems.at[0, i], w_sems.at[1, i], pair_dev)

    copy_rest = remote(
        mine_rest, peer_rest, w_sems.at[0, 2], w_sems.at[1, 2], pair_dev
    )

    def copy_acts(step):
        o = target(step)
        return remote(
            acts.at[1 - core, o], peer_acts.at[o],
            acts_sems.at[0, step], acts_sems.at[1, step], pair_dev,
        )

    def divide(step):
        o = target(step)
        load_acts(step).wait()
        for k in range(4):
            acts[k % 2, o, k // 2] = acts_raw[o, k * rows : (k + 1) * rows, :]

    load_wide[0].wait()
    mine[1 - half] = weigh(grad_raw[1 - half])
    pl.semaphore_wait(barrier, 4 + last)
    copy_wide(0).start()
    divide(0)
    copy_acts(0).start()
    for copy in load_rest:
        copy.wait()
    mine_rest[...] = weigh(rest_raw[...])
    copy_rest.start()
    load_wide[1].wait()
    mine[half] = weigh(grad_raw[half])
    copy_wide(1).start()

    def feed(step, carry):
        divide(step)
        copy_acts(step).start()
        return carry

    lax.fori_loop(1, outer, feed, 0)

    def contract(left, right):
        return lax.dot_general(
            left, right, (((1,), (1,)), ((), ())), preferred_element_type=jnp.float32
        )

    def term(step, a, b):
        o, m = target(step), b * (1 - core) + a * core
        column = a * (1 - core) + b * core
        return contract(acts[core, o, m], mine[column]) + contract(
            peer_acts[o, m], peer[column]
        )

    def rest_term(step):
        o = target(step)
        parts = [
            contract(mine_rest[...], acts[core, o, m])
            + contract(peer_rest[...], peer_acts[o, m])
            for m in range(2)
        ]
        return jnp.concatenate(parts, axis=1)

    def copy_a(step, k):
        return remote(
            send_a.at[step, k], recv_a.at[step, k],
            a_sems.at[0, step, k], a_sems.at[1, step, k], a_dev,
        )

    def copy_b(step):
        return remote(
            send_b.at[step], recv_b.at[step], b_sems.at[0, step], b_sems.at[1, step], b_dev
        )

    def copy_z(step):
        return remote(
            send_z.at[step], recv_z.at[step],
            z_sems.at[0, step], z_sems.at[1, step], z_dev(step),
        )

    def copy_r(step):
        return remote(
            send_r.at[step], recv_r.at[step],
            r_sems.at[0, step], r_sems.at[1, step], z_dev(step),
        )

    plane = (x_dev, y_dev, xy_dev)

    def copy_p(i):
        return remote(
            send_p.at[i], recv_p.at[i], p_sems.at[0, i], p_sems.at[1, i], plane[i]
        )

    def first(step, k):
        b = 1 - my_b if k == 0 else my_b
        send_a[step, k] = term(step, 1 - my_a, b).astype(jnp.bfloat16)
        copy_a(step, k).start()

    def rest_first(step):
        send_r[step] = rest_term(step).astype(jnp.bfloat16)
        copy_r(step).start()

    def second(step):
        total = term(step, my_a, 1 - my_b)
        copy_a(step, 0).wait_recv()
        total = total + recv_a[step, 0].astype(jnp.float32)
        send_b[step] = total.astype(jnp.bfloat16)
        copy_b(step).start()

    def third(step):
        total = term(step, my_a, my_b)
        copy_a(step, 1).wait_recv()
        total = total + recv_a[step, 1].astype(jnp.float32)
        copy_b(step).wait_recv()
        total = total + recv_b[step].astype(jnp.float32)
        send_z[step] = total.astype(jnp.bfloat16)
        copy_z(step).start()

    def rest_second():
        own_r[...] = rest_term(last)

        def add(step, carry):
            copy_r(step).wait_recv()
            own_r[...] += recv_r[step].astype(jnp.float32)
            return carry

        lax.fori_loop(0, last, add, 0)

        def piece(h):
            block = own_r[pl.ds(pl.multiple_of(h * rest, 16), rest), :]
            low, high = block[:, :rows], block[:, rows:]
            here = jnp.where(mid == 0, low, high)
            there = jnp.where(mid == 0, high, low)
            return here, there

        x_part, xy_part = piece(1 - half)
        mine_part, y_part = piece(half)
        for i, part in enumerate((x_part, y_part, xy_part)):
            send_p[i] = part.astype(jnp.bfloat16)
            copy_p(i).start()
        turned[...] = jnp.zeros_like(turned)
        turned[:rest, :rows] = mine_part

    def lead(step, both):
        copy_acts(step).wait_recv()
        first(step, 0)
        if both:
            copy_rest.wait_recv()

        @pl.when(step < last)
        def _():
            rest_first(step)

        if both:
            copy_wide(1).wait_recv()
        first(step, 1)

    copy_wide(0).wait_recv()
    lead(0, True)
    if outer > 1:
        lead(1, False)

    def stage(step, carry):
        @pl.when(step >= 1)
        def _():
            third(step - 1)

        second(step)

        @pl.when(step + 2 < outer)
        def _():
            lead(step + 2, False)

        @pl.when(step == min(1, last))
        def _():
            rest_second()

        return carry

    lax.fori_loop(0, outer, stage, 0)
    out_ref[:, :wide] = term(last, my_a, my_b)

    for i in range(3):
        copy_p(i).wait_recv()
        turned[:rest, :rows] += recv_p[i].astype(jnp.float32)
    out_ref[:, wide:] = turned[...].T[:rows, :rest]

    copy_a(last, 1).wait_recv()
    out_ref[:, :wide] += recv_a[last, 1].astype(jnp.float32)

    def add_z(step, carry):
        copy_z(step).wait_recv()
        out_ref[:, :wide] += recv_z[step].astype(jnp.float32)
        return carry

    lax.fori_loop(0, last, add_z, 0)
    copy_b(last).wait_recv()
    out_ref[:, :wide] += recv_b[last].astype(jnp.float32)

    def drain(step, carry):
        copy_acts(step).wait_send()
        copy_a(step, 0).wait_send()
        copy_a(step, 1).wait_send()
        copy_b(step).wait_send()
        return carry

    lax.fori_loop(0, outer, drain, 0)

    def drain_z(step, carry):
        copy_z(step).wait_send()
        copy_r(step).wait_send()
        return carry

    lax.fori_loop(0, last, drain_z, 0)
    copy_wide(0).wait_send()
    copy_wide(1).wait_send()
    copy_rest.wait_send()
    for i in range(3):
        copy_p(i).wait_send()


def shards(expert_act, grad_out, slot_token, slot_prob, live_count):
    slots, hidden = expert_act.shape
    tokens = grad_out.shape[0]
    ranks, halves = lax.axis_size("dp"), lax.axis_size("tensor")
    outer = ranks // 4
    rows, columns = hidden // ranks, grad_out.shape[1] // halves
    wide = columns // LANES * LANES
    rest = columns - wide
    scaling = 1.0 / math.sqrt(slots * ranks * halves)
    bf16, f32, dma = jnp.bfloat16, jnp.float32, pltpu.SemaphoreType.DMA
    anywhere = pl.BlockSpec(memory_space=pl.ANY)
    total = pl.pallas_call(
        functools.partial(kernel, outer, wide),
        out_shape=jax.ShapeDtypeStruct((rows, columns), f32),
        in_specs=[
            anywhere, anywhere, anywhere, anywhere,
            pl.BlockSpec(memory_space=pltpu.SMEM),
        ],
        out_specs=pl.BlockSpec(memory_space=pltpu.VMEM),
        scratch_shapes=[
            pltpu.VMEM((1, slots), jnp.int32),
            pltpu.VMEM((1, slots), f32),
            pltpu.VMEM((outer, 4 * rows, slots), bf16),
            pltpu.VMEM((halves, wide, tokens), bf16),
            pltpu.VMEM((halves * rest, tokens), bf16),
            pltpu.VMEM((2, outer, 2, rows, slots), bf16),
            pltpu.VMEM((outer, 2, rows, slots), bf16),
            pltpu.VMEM((halves, wide, slots), bf16),
            pltpu.VMEM((halves, wide, slots), bf16),
            pltpu.VMEM((halves * rest, slots), bf16),
            pltpu.VMEM((halves * rest, slots), bf16),
            pltpu.VMEM((outer, 2, rows, wide), bf16),
            pltpu.VMEM((outer, 2, rows, wide), bf16),
            pltpu.VMEM((outer, rows, wide), bf16),
            pltpu.VMEM((outer, rows, wide), bf16),
            pltpu.VMEM((outer - 1, rows, wide), bf16),
            pltpu.VMEM((outer - 1, rows, wide), bf16),
            pltpu.VMEM((outer - 1, halves * rest, 2 * rows), bf16),
            pltpu.VMEM((outer - 1, halves * rest, 2 * rows), bf16),
            pltpu.VMEM((halves * rest, 2 * rows), f32),
            pltpu.VMEM((3, rest, rows), bf16),
            pltpu.VMEM((3, rest, rows), bf16),
            pltpu.VMEM((pl.cdiv(rest, LANES) * LANES, pl.cdiv(rows, LANES) * LANES), f32),
            dma((2,)),
            dma((outer,)),
            dma((4,)),
            dma((2, outer)),
            dma((2, 3)),
            dma((2, outer, 2)),
            dma((2, outer)),
            dma((2, outer - 1)),
            dma((2, outer - 1)),
            dma((2, 3)),
        ],
        compiler_params=pltpu.CompilerParams(
            collective_id=0, has_side_effects=True, vmem_limit_bytes=53 * 2**20
        ),
    )(
        expert_act.T.reshape(outer, 4 * rows, slots),
        grad_out.T.reshape(halves, columns, tokens),
        slot_token[None, :],
        slot_prob[None, :],
        live_count,
    )
    return total * scaling


def solution(mesh):
    return jax.shard_map(
        shards,
        mesh=mesh,
        in_specs=(
            P(("dp", "tensor"), None),
            P(("dp", "tensor"), None),
            P(("dp", "tensor")),
            P(("dp", "tensor")),
            P(("dp", "tensor")),
        ),
        out_specs=P("dp", "tensor"),
        check_vma=False,
    )
```

```python
import functools
import math

import jax
import jax.numpy as jnp
from jax import lax
from jax.experimental import pallas as pl
from jax.experimental.pallas import tpu as pltpu
from jax.sharding import PartitionSpec as P

MESH = pl.DeviceIdType.MESH
PIECE = 256


def kernel(
    outer, columns,
    acts_hbm, grad_hbm, token_hbm, prob_hbm, live_ref, out_ref,
    token_ref, prob_ref, acts_raw, grad_raw, acts, peer_acts, mine, peer,
    send_a, recv_a, send_b, recv_b, send_z, recv_z, send_r, recv_r,
    small_sems, load_sems, grad_sems, acts_sems, w_sems,
    a_sems, b_sems, z_sems, r_sems,
):
    dp = lax.axis_index("dp")
    half = lax.axis_index("tensor")
    core = lax.rem(dp, 2)
    mid = lax.rem(dp // 2, 2)
    own = dp // 4
    my_a = half * (1 - core) + mid * core
    my_b = mid * (1 - core) + half * core
    flip_mid = dp + 2 - 4 * mid
    pair_dev = {"dp": dp + 1 - 2 * core, "tensor": half}
    a_dev = {
        "dp": dp * (1 - core) + flip_mid * core,
        "tensor": (1 - half) * (1 - core) + half * core,
    }
    b_dev = {
        "dp": flip_mid * (1 - core) + dp * core,
        "tensor": half * (1 - core) + (1 - half) * core,
    }
    side = lax.rem(own, 2)
    near = own + 1 - 2 * side
    pieces, rows = mine.shape[1], acts.shape[3]
    far_total = (outer - 2) * pieces
    total_pieces = far_total + 1 + pieces
    raws = send_r.shape[0]
    spots = ((1 - my_a, 1 - my_b), (1 - my_a, my_b), (my_a, 1 - my_b), (my_a, my_b))

    def far(j):
        pair = lax.rem(own // 2 + 1 + j // 2, outer // 2)
        return 2 * pair + lax.rem(side + j, 2)

    def place(i):
        is_far, is_near = i < far_total, i == far_total
        o = jnp.where(is_far, far(jnp.minimum(i, far_total - 1) // pieces), own)
        o = jnp.where(is_near, near, o)
        p = jnp.where(is_far, lax.rem(i, pieces), i - far_total - 1)
        return o, jnp.where(is_near, pieces - 1, p)

    def z_dev(o):
        return {"dp": dp + (o - own) * 4, "tensor": half}

    def remote(src, dst, sems, device):
        return pltpu.make_async_remote_copy(
            src_ref=src, dst_ref=dst, send_sem=sems[0], recv_sem=sems[1],
            device_id=device, device_id_type=MESH,
        )

    grad_order = (1 - half, half)
    act_order = [far(0), near] + [far(j) for j in range(1, outer - 2)] + [own]

    load_small = [
        pltpu.make_async_copy(token_hbm, token_ref, small_sems.at[0]),
        pltpu.make_async_copy(prob_hbm, prob_ref, small_sems.at[1]),
    ]

    def load_grad(p, i):
        window = pl.ds(p * PIECE, min(PIECE, columns - p * PIECE))
        g = grad_order[i]
        return pltpu.make_async_copy(
            grad_hbm.at[g, window], grad_raw.at[g, window], grad_sems.at[p, i]
        )

    def load_acts(o):
        return pltpu.make_async_copy(acts_hbm.at[o], acts_raw.at[o], load_sems.at[o])

    for copy in load_small:
        copy.start()
    load_grad(0, 0).start()
    load_acts(act_order[0]).start()
    load_grad(0, 1).start()
    load_acts(act_order[1]).start()
    for p in range(1, pieces):
        for i in range(2):
            load_grad(p, i).start()
    for o in act_order[2:]:
        load_acts(o).start()

    barrier = pltpu.get_barrier_semaphore()
    others = act_order[:-1]
    for device in [pair_dev, a_dev, b_dev] + [z_dev(o) for o in others]:
        pl.semaphore_signal(barrier, inc=1, device_id=device, device_id_type=MESH)

    slots, tokens = token_ref.shape[1], grad_raw.shape[2]
    if pieces * PIECE > columns:
        spare = pieces * PIECE - columns
        grad_raw[:, columns:] = jnp.zeros((2, spare, tokens), grad_raw.dtype)
    load_small[0].wait()
    load_small[1].wait()
    chosen = lax.broadcasted_iota(jnp.int32, (tokens, slots), 0) == token_ref[...]
    onehot = jnp.where(chosen, 1.0, 0.0).astype(jnp.bfloat16)
    live = lax.broadcasted_iota(jnp.int32, (1, slots), 1) < live_ref[0]
    weight = jnp.where(live, prob_ref[...], 0.0)

    def copy_w(p, i):
        g = grad_order[i]
        return remote(
            mine.at[g, p], peer.at[g, p],
            (w_sems.at[0, p, i], w_sems.at[1, p, i]), pair_dev,
        )

    def copy_acts(o):
        return remote(
            acts.at[1 - core, o], peer_acts.at[o],
            (acts_sems.at[0, o], acts_sems.at[1, o]), pair_dev,
        )

    def weigh(p, i):
        g = grad_order[i]
        load_grad(p, i).wait()
        picked = jnp.dot(
            grad_raw[g, p * PIECE : (p + 1) * PIECE], onehot,
            preferred_element_type=jnp.float32,
        )
        mine[g, p] = (picked * weight).astype(jnp.bfloat16)

    def divide(o):
        load_acts(o).wait()
        for k in range(4):
            acts[k % 2, o, k // 2] = acts_raw[o, k * rows : (k + 1) * rows, :]

    def contract(left, right):
        return lax.dot_general(
            left, right, (((1,), (1,)), ((), ())), preferred_element_type=jnp.float32
        )

    def term(o, p, spot):
        a, b = spot
        m = b * (1 - core) + a * core
        column = a * (1 - core) + b * core
        return contract(acts[core, o, m], mine[column, p]) + contract(
            peer_acts[o, m], peer[column, p]
        )

    def copy_a(i, k):
        return remote(
            send_a.at[i, k], recv_a.at[i, k],
            (a_sems.at[0, i, k], a_sems.at[1, i, k]), a_dev,
        )

    def copy_b(i):
        return remote(send_b.at[i], recv_b.at[i], (b_sems.at[0, i], b_sems.at[1, i]), b_dev)

    def copy_z(i):
        return remote(
            send_z.at[i], recv_z.at[i], (z_sems.at[0, i], z_sems.at[1, i]),
            z_dev(place(i)[0]),
        )

    def copy_r(r):
        return remote(
            send_r.at[r], recv_r.at[r], (r_sems.at[0, r], r_sems.at[1, r]), z_dev(near)
        )

    def with_raw(i, q, put, total):
        put(total)

        @pl.when((i > far_total) & (i < total_pieces - 1))
        def _():
            r = (i - far_total - 1) * 4 + q
            copy_r(r).wait_recv()
            put(total + recv_r[r].astype(jnp.float32))

    def first(i):
        o, p = place(i)
        for k in range(2):

            def put(total):
                send_a[i, k] = total.astype(jnp.bfloat16)

            with_raw(i, k, put, term(o, p, spots[k]))
            copy_a(i, k).start()

    def second(i):
        o, p = place(i)
        total = term(o, p, spots[2])
        copy_a(i, 0).wait_recv()

        def put(total):
            send_b[i] = total.astype(jnp.bfloat16)

        with_raw(i, 2, put, total + recv_a[i, 0].astype(jnp.float32))
        copy_b(i).start()

    def third(i):
        o, p = place(i)
        total = term(o, p, spots[3])
        copy_a(i, 1).wait_recv()
        total = total + recv_a[i, 1].astype(jnp.float32)
        copy_b(i).wait_recv()
        total = total + recv_b[i].astype(jnp.float32)
        send_z[i] = total.astype(jnp.bfloat16)
        copy_z(i).start()

    def raw(r):
        q = lax.rem(r, 4)
        a = jnp.where(q < 2, 1 - my_a, my_a)
        b = jnp.where(lax.rem(q, 2) == 0, 1 - my_b, my_b)
        send_r[r] = term(near, r // 4, (a, b)).astype(jnp.bfloat16)
        copy_r(r).start()

    weigh(0, 0)
    divide(act_order[0])
    pl.semaphore_wait(barrier, 2 + outer)
    copy_acts(act_order[0]).start()
    copy_w(0, 0).start()
    weigh(0, 1)
    copy_w(0, 1).start()
    divide(act_order[1])
    copy_acts(act_order[1]).start()
    for i in range(2):
        weigh(1, i)
        copy_w(1, i).start()
    copy_acts(act_order[0]).wait_recv()
    copy_w(0, 0).wait_recv()
    copy_w(0, 1).wait_recv()
    first(0)
    copy_acts(act_order[1]).wait_recv()
    raw(0)
    raw(1)
    for p in range(2, pieces):
        for i in range(2):
            weigh(p, i)
            copy_w(p, i).start()
    for o in act_order[2:]:
        divide(o)
        copy_acts(o).start()
    copy_w(1, 0).wait_recv()
    copy_w(1, 1).wait_recv()
    first(1)
    raw(2)
    for p in range(2, pieces):
        for i in range(2):
            copy_w(p, i).wait_recv()
    for o in act_order[2:]:
        copy_acts(o).wait_recv()

    def stage(i, carry):
        second(i)

        @pl.when(i + 2 < total_pieces)
        def _():
            first(i + 2)

        @pl.when(i + 3 < raws)
        def _():
            raw(i + 3)

        @pl.when((i >= 1) & (i - 1 <= far_total))
        def _():
            third(i - 1)

        return carry

    lax.fori_loop(0, total_pieces, stage, 0)

    for p in range(pieces):
        i = far_total + 1 + p
        width = min(PIECE, columns - p * PIECE)
        total = term(own, p, spots[3])
        if p < pieces - 1:
            copy_r(p * 4 + 3).wait_recv()
            total = total + recv_r[p * 4 + 3].astype(jnp.float32)
        copy_a(i, 1).wait_recv()
        total = total + recv_a[i, 1].astype(jnp.float32)
        for j in range(outer - 2):
            copy_z(j * pieces + p).wait_recv()
            total = total + recv_z[j * pieces + p].astype(jnp.float32)
        copy_b(i).wait_recv()
        total = total + recv_b[i].astype(jnp.float32)
        if p == pieces - 1:
            copy_z(far_total).wait_recv()
            total = total + recv_z[far_total].astype(jnp.float32)
        out_ref[:, p * PIECE : p * PIECE + width] = total[:, :width]

    def drain(i, carry):
        copy_a(i, 0).wait_send()
        copy_a(i, 1).wait_send()
        copy_b(i).wait_send()
        return carry

    lax.fori_loop(0, total_pieces, drain, 0)

    def drain_z(i, carry):
        copy_z(i).wait_send()
        return carry

    lax.fori_loop(0, far_total + 1, drain_z, 0)

    def drain_r(r, carry):
        copy_r(r).wait_send()
        return carry

    lax.fori_loop(0, raws, drain_r, 0)
    for p in range(pieces):
        for i in range(2):
            copy_w(p, i).wait_send()
    for o in act_order:
        copy_acts(o).wait_send()


def shards(expert_act, grad_out, slot_token, slot_prob, live_count):
    slots, hidden = expert_act.shape
    tokens = grad_out.shape[0]
    ranks, halves = lax.axis_size("dp"), lax.axis_size("tensor")
    outer = ranks // 4
    rows, columns = hidden // ranks, grad_out.shape[1] // halves
    pieces = pl.cdiv(columns, PIECE)
    count = (outer - 1) * pieces + 1
    raws = 4 * (pieces - 1)
    scaling = 1.0 / math.sqrt(slots * ranks * halves)
    bf16, f32, dma = jnp.bfloat16, jnp.float32, pltpu.SemaphoreType.DMA
    anywhere = pl.BlockSpec(memory_space=pl.ANY)
    total = pl.pallas_call(
        functools.partial(kernel, outer, columns),
        out_shape=jax.ShapeDtypeStruct((rows, columns), f32),
        in_specs=[
            anywhere, anywhere, anywhere, anywhere,
            pl.BlockSpec(memory_space=pltpu.SMEM),
        ],
        out_specs=pl.BlockSpec(memory_space=pltpu.VMEM),
        scratch_shapes=[
            pltpu.VMEM((1, slots), jnp.int32),
            pltpu.VMEM((1, slots), f32),
            pltpu.VMEM((outer, 4 * rows, slots), bf16),
            pltpu.VMEM((halves, pieces * PIECE, tokens), bf16),
            pltpu.VMEM((2, outer, 2, rows, slots), bf16),
            pltpu.VMEM((outer, 2, rows, slots), bf16),
            pltpu.VMEM((halves, pieces, PIECE, slots), bf16),
            pltpu.VMEM((halves, pieces, PIECE, slots), bf16),
            pltpu.VMEM((count, 2, rows, PIECE), bf16),
            pltpu.VMEM((count, 2, rows, PIECE), bf16),
            pltpu.VMEM((count, rows, PIECE), bf16),
            pltpu.VMEM((count, rows, PIECE), bf16),
            pltpu.VMEM((count - pieces, rows, PIECE), bf16),
            pltpu.VMEM((count - pieces, rows, PIECE), bf16),
            pltpu.VMEM((raws, rows, PIECE), bf16),
            pltpu.VMEM((raws, rows, PIECE), bf16),
            dma((2,)),
            dma((outer,)),
            dma((pieces, 2)),
            dma((2, outer)),
            dma((2, pieces, 2)),
            dma((2, count, 2)),
            dma((2, count)),
            dma((2, count - pieces)),
            dma((2, raws)),
        ],
        compiler_params=pltpu.CompilerParams(
            collective_id=0, has_side_effects=True, vmem_limit_bytes=53 * 2**20
        ),
    )(
        expert_act.T.reshape(outer, 4 * rows, slots),
        grad_out.T.reshape(halves, columns, tokens),
        slot_token[None, :],
        slot_prob[None, :],
        live_count,
    )
    return total * scaling


def solution(mesh):
    return jax.shard_map(
        shards,
        mesh=mesh,
        in_specs=(
            P(("dp", "tensor"), None),
            P(("dp", "tensor"), None),
            P(("dp", "tensor")),
            P(("dp", "tensor")),
            P(("dp", "tensor")),
        ),
        out_specs=P("dp", "tensor"),
        check_vma=False,
    )
```

```python
import functools
import math

import jax
import jax.numpy as jnp
from jax import lax
from jax.experimental import pallas as pl
from jax.experimental.pallas import tpu as pltpu
from jax.sharding import PartitionSpec as P

MESH = pl.DeviceIdType.MESH
PIECE = 256
LANES = 128


TUNED = (2, 3)
ORDER = (
    "F000", "X000", "G00", "N0", "R0", "X010", "X020", "F01", "X001",
    "H02", "S00", "X011", "N1", "S01", "R1", "H03", "X021", "F10",
    "S02", "F11", "H12", "T00", "X100", "H13", "N2", "X110", "N3",
    "T01", "F30", "X120", "H32", "T02", "X101", "R2", "F31", "S10",
    "X111", "H33", "S11", "X121", "S12", "Y00", "X220", "T10", "Y01",
    "X221", "T11", "X300", "Y02", "X310", "T12", "R3", "S22", "X320",
    "Y10", "X301", "S30", "X311", "T22", "Y11", "S31", "X321", "Y12",
    "S32",
)


def plan(fars, pieces):
    if (fars, pieces) == TUNED:
        return [(token[0], *map(int, token[1:])) for token in ORDER]
    near, own, every = fars, fars + 1, range(pieces)
    steps = [("F", 0, 0, p) for p in every] + [("F", 0, 1, p) for p in every]
    steps += [("X", 0, p, k) for k in range(2) for p in every]
    steps += [(name, q) for q in range(4) for name in "NR"]
    steps += [("X", near, pieces - 1, k) for k in range(2)]
    for j in list(range(fars)) + [near, own]:
        then = j + 1 if j + 1 < fars else own
        if j < near:
            steps += [("F", then, k, p) for k in range(2) for p in every]
            steps += [("H", j, 2), ("H", j, 3)]
        if j == own:
            steps += [("H", j, 2), ("H", j, 3)]
        mine = [pieces - 1] if j == near else every
        steps += [("S", j, p) for p in mine]
        if j < near:
            steps += [("X", then, p, k) for k in range(2) for p in every]
        if j < own:
            steps += [("T", j, p) for p in mine]
        if j < near:
            steps += [("Y", j, p) for p in every]
    return steps


def kernel(
    outer,
    acts_hbm, grad_hbm, token_ref, prob_ref, live_ref, out_ref,
    acts_raw, grad_raw, acts, peer_acts, mine, peer, onehot, weight, held,
    send_a, recv_a, send_b, recv_b, send_z, recv_z, recv_y, send_r, recv_r,
    load_sems, grad_sems, acts_sems, w_sems,
    a_sems, b_sems, z_sems, y_sems, r_sems,
):
    dp = lax.axis_index("dp")
    half = lax.axis_index("tensor")
    core = lax.rem(dp, 2)
    mid = lax.rem(dp // 2, 2)
    own = dp // 4
    my_a = half * (1 - core) + mid * core
    my_b = mid * (1 - core) + half * core
    flip_mid = dp + 2 - 4 * mid
    pair_dev = {"dp": dp + 1 - 2 * core, "tensor": half}
    a_dev = {
        "dp": dp * (1 - core) + flip_mid * core,
        "tensor": (1 - half) * (1 - core) + half * core,
    }
    b_dev = {
        "dp": flip_mid * (1 - core) + dp * core,
        "tensor": half * (1 - core) + (1 - half) * core,
    }
    side = lax.rem(own, 2)
    near = own + 1 - 2 * side
    columns, pieces = out_ref.shape[1], mine.shape[2] // PIECE
    rows, slots = acts.shape[3], acts.shape[4]
    tokens = grad_raw.shape[2]
    fars = outer - 2
    far_total = fars * pieces
    raws = send_r.shape[0]
    spots = ((1 - my_a, 1 - my_b), (1 - my_a, my_b), (my_a, 1 - my_b), (my_a, my_b))

    def far_pair(j):
        pair = lax.rem(own // 2 + 1 + j // 2, outer // 2)
        return pair, jnp.where(pair > own // 2, 1, 0)

    def far(j):
        pair, up = far_pair(j)
        return 2 * pair + (up if j % 2 == 0 else 1 - up)

    def leads(j):
        return side == far_pair(j)[1]

    targets = [far(j) for j in range(fars)] + [near, own]
    NEAR, OWN = fars, fars + 1

    def z_dev(o):
        return {"dp": dp + (o - own) * 4, "tensor": half}

    def remote(src, dst, sems, device):
        return pltpu.make_async_remote_copy(
            src_ref=src, dst_ref=dst, send_sem=sems[0], recv_sem=sems[1],
            device_id=device, device_id_type=MESH,
        )

    grad_order = (1 - half, half)

    def load_grad(i, j):
        g = grad_order[i]
        window = pl.ds(0, PIECE) if j == 0 else pl.ds(PIECE, columns - PIECE)
        return pltpu.make_async_copy(
            grad_hbm.at[g, window], grad_raw.at[g, window], grad_sems.at[i, j]
        )

    def load_acts(step):
        o = targets[step]
        return pltpu.make_async_copy(acts_hbm.at[o], acts_raw.at[o], load_sems.at[step])

    act_order = [0, NEAR] + list(range(1, fars)) + [OWN]
    load_grad(0, 0).start()
    load_acts(act_order[0]).start()
    load_grad(0, 1).start()
    load_acts(act_order[1]).start()
    for j in range(2):
        load_grad(1, j).start()
    for step in act_order[2:]:
        load_acts(step).start()

    barrier = pltpu.get_barrier_semaphore()
    for device in [pair_dev, a_dev, b_dev] + [z_dev(o) for o in targets[:OWN]]:
        pl.semaphore_signal(barrier, inc=1, device_id=device, device_id_type=MESH)

    def turn(row):
        return jnp.broadcast_to(row.astype(jnp.float32), (LANES, slots)).T

    token = turn(token_ref[...])
    lane = lax.broadcasted_iota(jnp.int32, (slots, LANES), 1).astype(jnp.float32)
    for t in range(0, tokens, LANES):
        onehot[:, t : t + LANES] = jnp.where(token - t == lane, 1.0, 0.0).astype(
            onehot.dtype
        )
    live = lax.broadcasted_iota(jnp.int32, (1, slots), 1) < live_ref[0]
    weight[...] = turn(jnp.where(live, prob_ref[...], 0.0))
    if pieces * PIECE > columns:
        ragged = columns // LANES * LANES
        mine[:, :, ragged:] = jnp.zeros(
            (2, slots, pieces * PIECE - ragged), mine.dtype
        )

    def span(p):
        return slice(p * PIECE, (p + 1) * PIECE)

    def copy_w(i, p):
        g = grad_order[i]
        return remote(
            mine.at[g, :, pl.ds(p * PIECE, PIECE)],
            peer.at[g, :, pl.ds(p * PIECE, PIECE)],
            (w_sems.at[0, i, p], w_sems.at[1, i, p]), pair_dev,
        )

    def copy_acts(step):
        o = targets[step]
        return remote(
            acts.at[1 - core, o], peer_acts.at[o],
            (acts_sems.at[0, step], acts_sems.at[1, step]), pair_dev,
        )

    def weigh(i, begin, end):
        g = grad_order[i]
        picked = lax.dot_general(
            onehot[...], grad_raw[g, begin:end], (((1,), (1,)), ((), ())),
            preferred_element_type=jnp.float32,
        )
        for t in range(begin, end, LANES):
            stop = min(t + LANES, end)
            mine[g, :, t:stop] = (
                picked[:, t - begin : stop - begin] * weight[:, : stop - t]
            ).astype(jnp.bfloat16)

    def divide(step):
        o = targets[step]
        load_acts(step).wait()
        for k in range(4):
            acts[k % 2, o, k // 2] = acts_raw[o, k * rows : (k + 1) * rows, :]

    def contract(left, right):
        return jnp.dot(left, right, preferred_element_type=jnp.float32)

    def term(step, q, window=slice(None)):
        o = targets[step]
        a, b = spots[q]
        m = b * (1 - core) + a * core
        column = a * (1 - core) + b * core
        return contract(acts[core, o, m], mine[column, :, window]) + contract(
            peer_acts[o, m], peer[column, :, window]
        )

    def index(step, p):
        return step * pieces + p if step < NEAR else far_total + (0 if step == NEAR else 1 + p)

    def copy_a(step, p, k):
        i = index(step, p)
        return remote(
            send_a.at[i, k], recv_a.at[i, k],
            (a_sems.at[0, i, k], a_sems.at[1, i, k]), a_dev,
        )

    def copy_b(step, p):
        i = index(step, p)
        return remote(send_b.at[i], recv_b.at[i], (b_sems.at[0, i], b_sems.at[1, i]), b_dev)

    def slot(step, p):
        return step // 2 * pieces + p if step < NEAR else fars // 2 * pieces

    def copy_z(step, p):
        i, j = index(step, p), slot(step, p)
        return remote(
            send_z.at[i], recv_z.at[j], (z_sems.at[0, i], z_sems.at[1, j]),
            z_dev(targets[step]),
        )

    def copy_y(step, p):
        i = index(step, p)
        return remote(
            send_z.at[i], recv_y.at[i], (z_sems.at[0, i], y_sems.at[i]), z_dev(near)
        )

    def copy_r(r):
        return remote(
            send_r.at[r], recv_r.at[r], (r_sems.at[0, r], r_sems.at[1, r]), z_dev(near)
        )

    def raw_in(p, q):
        r = p * 4 + q
        copy_r(r).wait_recv()
        return recv_r[r].astype(jnp.float32)

    def wide(ref):
        return ref[...].astype(jnp.float32)

    seen = set()

    def need(step, q, pieces_end):
        wanted = [copy_acts(step)] if ("acts", step) not in seen else []
        seen.add(("acts", step))
        for i in range(1 if q == 0 else 2):
            for p in range(pieces_end):
                if (i, p) not in seen:
                    seen.add((i, p))
                    wanted.append(copy_w(i, p))
        for copy in wanted:
            copy.wait_recv()

    def first(step, k, p=None):
        begin, end = (0, pieces) if p is None else (p, p + 1)
        need(step, k, end)
        total = term(step, k, slice(begin * PIECE, end * PIECE))
        for p in range(begin, end):
            part = total[:, span(p - begin)]
            if step == OWN and p < pieces - 1:
                part = part + raw_in(p, k)
            send_a[index(step, p), k] = part.astype(jnp.bfloat16)

    def first_rest(step, k):
        need(step, k, pieces)
        total = term(step, k, slice(PIECE, pieces * PIECE))
        for p in range(1, pieces):
            send_a[index(step, p), k] = total[:, span(p - 1)].astype(jnp.bfloat16)

    def send_first(step, p, k):
        copy_a(step, p, k).start()

    def near_all(q):
        need(NEAR, q, pieces)
        total = term(NEAR, q)
        for p in range(pieces - 1):
            send_r[p * 4 + q] = total[:, span(p)].astype(jnp.bfloat16)
        p = pieces - 1
        part = total[:, span(p)]
        if q < 2:
            send_a[index(NEAR, p), q] = part.astype(jnp.bfloat16)
        else:
            held[NEAR, q - 2, :, span(p)] = part

    def send_raw(q):
        for p in range(pieces - 1):
            copy_r(p * 4 + q).start()

    def hold(step, q):
        need(step, q, pieces)
        held[step, q - 2] = term(step, q)

    def second(step, p):
        copy_a(step, p, 0).wait_recv()
        total = held[step, 0, :, span(p)] + wide(recv_a.at[index(step, p), 0])
        if step == OWN and p < pieces - 1:
            total = total + raw_in(p, 2)
        send_b[index(step, p)] = total.astype(jnp.bfloat16)
        copy_b(step, p).start()

    def third(step, p):
        copy_a(step, p, 1).wait_recv()
        copy_b(step, p).wait_recv()
        i = index(step, p)
        total = held[step, 1, :, span(p)] + wide(recv_a.at[i, 1]) + wide(recv_b.at[i])
        if step == NEAR:
            send_z[i] = total.astype(jnp.bfloat16)
            copy_z(step, p).start()
            return

        @pl.when(leads(step))
        def _():
            held[step, 1, :, span(p)] = total

        @pl.when(jnp.logical_not(leads(step)))
        def _():
            send_z[i] = total.astype(jnp.bfloat16)
            copy_y(step, p).start()

    def forward(step, p):
        i = index(step, p)

        @pl.when(leads(step))
        def _():
            copy_y(step, p).wait_recv()
            total = held[step, 1, :, span(p)] + wide(recv_y.at[i])
            send_z[i] = total.astype(jnp.bfloat16)
            copy_z(step, p).start()

    load_grad(0, 0).wait()
    weigh(0, 0, PIECE)
    divide(act_order[0])
    pl.semaphore_wait(barrier, 2 + outer)
    copy_acts(act_order[0]).start()
    copy_w(0, 0).start()
    load_grad(0, 1).wait()
    weigh(0, PIECE, columns)
    for p in range(1, pieces):
        copy_w(0, p).start()
    divide(NEAR)
    copy_acts(NEAR).start()
    for j in range(2):
        load_grad(1, j).wait()
    weigh(1, 0, columns)
    for p in range(pieces):
        copy_w(1, p).start()
    for step in act_order[2:]:
        divide(step)
        copy_acts(step).start()
    actions = {
        "F": first, "G": first_rest, "X": send_first, "N": near_all, "R": send_raw,
        "H": hold, "S": second, "T": third, "Y": forward,
    }
    for name, *where in plan(fars, pieces):
        actions[name](*where)

    for step in range(outer):
        for p in range(pieces):
            if step == NEAR and p < pieces - 1:
                continue
            copy_a(step, p, 0).wait_send()
            copy_a(step, p, 1).wait_send()
            if step < NEAR:
                copy_b(step, p).wait_send()
        copy_acts(step).wait_send()
    for r in range(raws):
        copy_r(r).wait_send()
    for i in range(2):
        for p in range(pieces):
            copy_w(i, p).wait_send()

    for p in range(pieces):
        i = index(OWN, p)
        width = min(PIECE, columns - p * PIECE)
        total = held[OWN, 1, :, span(p)]
        if p < pieces - 1:
            total = total + raw_in(p, 3)
        copy_a(OWN, p, 1).wait_recv()
        total = total + wide(recv_a.at[i, 1])
        held[OWN, 1, :, span(p)] = total
    for p in range(pieces):
        i = index(OWN, p)
        width = min(PIECE, columns - p * PIECE)
        copy_b(OWN, p).wait_recv()
        total = held[OWN, 1, :, span(p)] + wide(recv_b.at[i])
        for step in range(0, fars, 2):
            copy_z(step, p).wait_recv()
            total = total + wide(recv_z.at[slot(step, p)])
        if p == pieces - 1:
            copy_z(NEAR, p).wait_recv()
            total = total + wide(recv_z.at[slot(NEAR, p)])
        out_ref[:, p * PIECE : p * PIECE + width] = total[:, :width]
        copy_b(OWN, p).wait_send()
    for step in range(fars):
        for p in range(pieces):
            copy_z(step, p).wait_send()
    copy_b(NEAR, pieces - 1).wait_send()
    copy_z(NEAR, pieces - 1).wait_send()


def shards(expert_act, grad_out, slot_token, slot_prob, live_count):
    slots, hidden = expert_act.shape
    tokens = grad_out.shape[0]
    ranks, halves = lax.axis_size("dp"), lax.axis_size("tensor")
    outer = ranks // 4
    rows, columns = hidden // ranks, grad_out.shape[1] // halves
    pieces = pl.cdiv(columns, PIECE)
    count = (outer - 1) * pieces + 1
    raws = 4 * (pieces - 1)
    scaling = 1.0 / math.sqrt(slots * ranks * halves)
    bf16, f32, dma = jnp.bfloat16, jnp.float32, pltpu.SemaphoreType.DMA
    anywhere = pl.BlockSpec(memory_space=pl.ANY)
    total = pl.pallas_call(
        functools.partial(kernel, outer),
        out_shape=jax.ShapeDtypeStruct((rows, columns), f32),
        in_specs=[
            anywhere,
            anywhere,
            pl.BlockSpec(memory_space=pltpu.VMEM),
            pl.BlockSpec(memory_space=pltpu.VMEM),
            pl.BlockSpec(memory_space=pltpu.SMEM),
        ],
        out_specs=pl.BlockSpec(memory_space=pltpu.VMEM),
        scratch_shapes=[
            pltpu.VMEM((outer, 4 * rows, slots), bf16),
            pltpu.VMEM((halves, columns, tokens), bf16),
            pltpu.VMEM((2, outer, 2, rows, slots), bf16),
            pltpu.VMEM((outer, 2, rows, slots), bf16),
            pltpu.VMEM((halves, slots, pieces * PIECE), bf16),
            pltpu.VMEM((halves, slots, pieces * PIECE), bf16),
            pltpu.VMEM((slots, tokens), bf16),
            pltpu.VMEM((slots, LANES), f32),
            pltpu.VMEM((outer, 2, rows, pieces * PIECE), f32),
            pltpu.VMEM((count, 2, rows, PIECE), bf16),
            pltpu.VMEM((count, 2, rows, PIECE), bf16),
            pltpu.VMEM((count, rows, PIECE), bf16),
            pltpu.VMEM((count, rows, PIECE), bf16),
            pltpu.VMEM((count - pieces, rows, PIECE), bf16),
            pltpu.VMEM((count - pieces, rows, PIECE), bf16),
            pltpu.VMEM((count - pieces, rows, PIECE), bf16),
            pltpu.VMEM((raws, rows, PIECE), bf16),
            pltpu.VMEM((raws, rows, PIECE), bf16),
            dma((outer,)),
            dma((2, 2)),
            dma((2, outer)),
            dma((2, 2, pieces)),
            dma((2, count, 2)),
            dma((2, count)),
            dma((2, count - pieces)),
            dma((count - pieces,)),
            dma((2, raws)),
        ],
        compiler_params=pltpu.CompilerParams(
            collective_id=0, has_side_effects=True, vmem_limit_bytes=53 * 2**20
        ),
    )(
        expert_act.T.reshape(outer, 4 * rows, slots),
        grad_out.T.reshape(halves, columns, tokens),
        slot_token[None, :],
        slot_prob[None, :],
        live_count,
    )
    return total * scaling


def solution(mesh):
    return jax.shard_map(
        shards,
        mesh=mesh,
        in_specs=(
            P(("dp", "tensor"), None),
            P(("dp", "tensor"), None),
            P(("dp", "tensor")),
            P(("dp", "tensor")),
            P(("dp", "tensor")),
        ),
        out_specs=P("dp", "tensor"),
        check_vma=False,
    )
```

```python
import functools
import math

import jax
import jax.numpy as jnp
from jax import lax
from jax.experimental import pallas as pl
from jax.experimental.pallas import tpu as pltpu
from jax.sharding import PartitionSpec as P

MESH = pl.DeviceIdType.MESH
PIECE = 256
LANES = 128


TUNED = (2, 3)
ORDER = (
    "F000", "X000", "N001", "R001", "G00", "X010", "X020", "M0", "R01",
    "F01", "X001", "H02", "S00", "X011", "N1", "S01", "R1", "H03",
    "X021", "F10", "S02", "F11", "H12", "T00", "X100", "H13", "N2",
    "X110", "N3", "T01", "F30", "X120", "H32", "T02", "X101", "R2",
    "F31", "S10", "X111", "H33", "S11", "X121", "S12", "Y00", "X220",
    "X221", "T10", "Y01", "X300", "X310", "T11", "X320", "Y02", "X301",
    "T12", "R3", "X311", "S22", "S30", "X321", "Y10", "T22", "S31",
    "Y11", "Y12", "S32",
)


def plan(fars, pieces):
    if (fars, pieces) == TUNED:
        return [(token[0], *map(int, token[1:])) for token in ORDER]
    near, own, every = fars, fars + 1, range(pieces)
    steps = [("F", 0, 0, p) for p in every] + [("F", 0, 1, p) for p in every]
    steps += [("X", 0, p, k) for k in range(2) for p in every]
    steps += [(name, q) for q in range(4) for name in "NR"]
    steps += [("X", near, pieces - 1, k) for k in range(2)]
    for j in list(range(fars)) + [near, own]:
        then = j + 1 if j + 1 < fars else own
        if j < near:
            steps += [("F", then, k, p) for k in range(2) for p in every]
            steps += [("H", j, 2), ("H", j, 3)]
        if j == own:
            steps += [("H", j, 2), ("H", j, 3)]
        mine = [pieces - 1] if j == near else every
        steps += [("S", j, p) for p in mine]
        if j < near:
            steps += [("X", then, p, k) for k in range(2) for p in every]
        if j < own:
            steps += [("T", j, p) for p in mine]
        if j < near:
            steps += [("Y", j, p) for p in every]
    return steps


def kernel(
    outer,
    acts_hbm, grad_hbm, token_ref, prob_ref, live_ref, out_ref,
    acts_raw, grad_raw, acts, peer_acts, mine, peer, onehot, weight, held,
    send_a, recv_a, send_b, recv_b, send_z, recv_z, recv_y, send_r, recv_r,
    load_sems, grad_sems, acts_sems, w_sems,
    a_sems, b_sems, z_sems, y_sems, r_sems, sent, ready,
):
    dp = lax.axis_index("dp")
    half = lax.axis_index("tensor")
    core = lax.rem(dp, 2)
    mid = lax.rem(dp // 2, 2)
    own = dp // 4
    my_a = half * (1 - core) + mid * core
    my_b = mid * (1 - core) + half * core
    flip_mid = dp + 2 - 4 * mid
    pair_dev = {"dp": dp + 1 - 2 * core, "tensor": half}
    a_dev = {
        "dp": dp * (1 - core) + flip_mid * core,
        "tensor": (1 - half) * (1 - core) + half * core,
    }
    b_dev = {
        "dp": flip_mid * (1 - core) + dp * core,
        "tensor": half * (1 - core) + (1 - half) * core,
    }
    side = lax.rem(own, 2)
    near = own + 1 - 2 * side
    columns, pieces = out_ref.shape[1], mine.shape[2] // PIECE
    rows, slots = acts.shape[3], acts.shape[4]
    tokens = grad_raw.shape[2]
    fars = outer - 2
    far_total = fars * pieces
    raws = send_r.shape[0]
    spots = ((1 - my_a, 1 - my_b), (1 - my_a, my_b), (my_a, 1 - my_b), (my_a, my_b))

    def far_pair(j):
        pair = lax.rem(own // 2 + 1 + j // 2, outer // 2)
        return pair, jnp.where(pair > own // 2, 1, 0)

    def far(j):
        pair, up = far_pair(j)
        return 2 * pair + (up if j % 2 == 0 else 1 - up)

    def leads(j):
        return side == far_pair(j)[1]

    targets = [far(j) for j in range(fars)] + [near, own]
    NEAR, OWN = fars, fars + 1

    def z_dev(o):
        return {"dp": dp + (o - own) * 4, "tensor": half}

    def remote(src, dst, sems, device):
        return pltpu.make_async_remote_copy(
            src_ref=src, dst_ref=dst, send_sem=sems[0], recv_sem=sems[1],
            device_id=device, device_id_type=MESH,
        )

    grad_order = (1 - half, half)

    def load_grad(i, j):
        g = grad_order[i]
        window = pl.ds(0, PIECE) if j == 0 else pl.ds(PIECE, columns - PIECE)
        return pltpu.make_async_copy(
            grad_hbm.at[g, window], grad_raw.at[g, window], grad_sems.at[i, j]
        )

    def load_acts(step):
        o = targets[step]
        return pltpu.make_async_copy(acts_hbm.at[o], acts_raw.at[o], load_sems.at[step])

    act_order = [0, NEAR] + list(range(1, fars)) + [OWN]
    load_grad(0, 0).start()
    load_acts(act_order[0]).start()
    load_grad(0, 1).start()
    load_acts(act_order[1]).start()
    for j in range(2):
        load_grad(1, j).start()
    for step in act_order[2:]:
        load_acts(step).start()

    barrier = pltpu.get_barrier_semaphore()
    relayed = fars == 2
    greet = [pair_dev, a_dev, b_dev, z_dev(near)]
    if not relayed:
        greet += [z_dev(o) for o in targets[:NEAR]]
    for device in greet:
        pl.semaphore_signal(barrier, inc=1, device_id=device, device_id_type=MESH)

    def tell_inner(semaphore):
        @pl.when(leads(0))
        def _():
            pl.semaphore_signal(
                semaphore, inc=1, device_id=z_dev(far(1)), device_id_type=MESH
            )

    if relayed:
        tell_inner(barrier)

    def turn(row):
        return jnp.broadcast_to(row.astype(jnp.float32), (LANES, slots)).T

    token = turn(token_ref[...])
    lane = lax.broadcasted_iota(jnp.int32, (slots, LANES), 1).astype(jnp.float32)
    for t in range(0, tokens, LANES):
        onehot[:, t : t + LANES] = jnp.where(token - t == lane, 1.0, 0.0).astype(
            onehot.dtype
        )
    live = lax.broadcasted_iota(jnp.int32, (1, slots), 1) < live_ref[0]
    weight[...] = turn(jnp.where(live, prob_ref[...], 0.0))
    if pieces * PIECE > columns:
        ragged = columns // LANES * LANES
        mine[:, :, ragged:] = jnp.zeros(
            (2, slots, pieces * PIECE - ragged), mine.dtype
        )

    def span(p):
        return slice(p * PIECE, (p + 1) * PIECE)

    def copy_w(i, p):
        g = grad_order[i]
        return remote(
            mine.at[g, :, pl.ds(p * PIECE, PIECE)],
            peer.at[g, :, pl.ds(p * PIECE, PIECE)],
            (sent.at[1], w_sems.at[i, p]), pair_dev,
        )

    def copy_acts(step, far_half):
        o, m = targets[step], 1 - mid if far_half else mid
        return remote(
            acts.at[1 - core, o, m], peer_acts.at[o, m],
            (sent.at[0], acts_sems.at[step, far_half]), pair_dev,
        )

    def send_acts(step):
        for far_half in (1, 0):
            copy_acts(step, far_half).start()

    def weigh(i, begin, end):
        g = grad_order[i]
        picked = lax.dot_general(
            onehot[...], grad_raw[g, begin:end], (((1,), (1,)), ((), ())),
            preferred_element_type=jnp.float32,
        )
        for t in range(begin, end, LANES):
            stop = min(t + LANES, end)
            mine[g, :, t:stop] = (
                picked[:, t - begin : stop - begin] * weight[:, : stop - t]
            ).astype(jnp.bfloat16)

    def divide(step):
        o = targets[step]
        load_acts(step).wait()
        for k in range(4):
            acts[k % 2, o, k // 2] = acts_raw[o, k * rows : (k + 1) * rows, :]

    def contract(left, right):
        return jnp.dot(left, right, preferred_element_type=jnp.float32)

    def term(step, q, window=slice(None)):
        o = targets[step]
        a, b = spots[q]
        m = b * (1 - core) + a * core
        column = a * (1 - core) + b * core
        return contract(acts[core, o, m], mine[column, :, window]) + contract(
            peer_acts[o, m], peer[column, :, window]
        )

    def index(step, p):
        return step * pieces + p if step < NEAR else far_total + (0 if step == NEAR else 1 + p)

    def copy_a(step, p, k):
        i = index(step, p)
        return remote(
            send_a.at[i, k], recv_a.at[i, k],
            (sent.at[2], a_sems.at[i, k]), a_dev,
        )

    def copy_b(step, p):
        i = index(step, p)
        return remote(send_b.at[i], recv_b.at[i], (sent.at[3], b_sems.at[i]), b_dev)

    def slot(step, p):
        return step // 2 * pieces + p if step < NEAR else fars // 2 * pieces

    def copy_z(step, p):
        i, j = index(step, p), slot(step, p)
        return remote(
            send_z.at[i], recv_z.at[j], (sent.at[4], z_sems.at[j]),
            z_dev(targets[step]),
        )

    def copy_y(step, p):
        i = index(step, p)
        return remote(
            send_z.at[i], recv_y.at[i], (sent.at[4], y_sems.at[i]), z_dev(near)
        )

    def copy_r(r):
        return remote(
            send_r.at[r], recv_r.at[r], (sent.at[5], r_sems.at[r]), z_dev(near)
        )

    def raw_in(p, q):
        r = p * 4 + q
        copy_r(r).wait_recv()
        return recv_r[r].astype(jnp.float32)

    def wide(ref):
        return ref[...].astype(jnp.float32)

    seen = set()

    def need(step, q, pieces_end):
        wanted = []
        for far_half in (1,) if q == 0 else (1, 0):
            if ("acts", step, far_half) not in seen:
                seen.add(("acts", step, far_half))
                wanted.append(copy_acts(step, far_half))
        for i in range(1 if q == 0 else 2):
            for p in range(pieces_end):
                if (i, p) not in seen:
                    seen.add((i, p))
                    wanted.append(copy_w(i, p))
        for copy in wanted:
            copy.wait_recv()

    def first(step, k, p=None):
        begin, end = (0, pieces) if p is None else (p, p + 1)
        need(step, k, end)
        total = term(step, k, slice(begin * PIECE, end * PIECE))
        for p in range(begin, end):
            part = total[:, span(p - begin)]
            if step == OWN and p < pieces - 1:
                part = part + raw_in(p, k)
            send_a[index(step, p), k] = part.astype(jnp.bfloat16)

    def first_rest(step, k):
        need(step, k, pieces)
        total = term(step, k, slice(PIECE, pieces * PIECE))
        for p in range(1, pieces):
            send_a[index(step, p), k] = total[:, span(p - 1)].astype(jnp.bfloat16)

    def send_first(step, p, k):
        copy_a(step, p, k).start()

    def near_some(q, begin=0, end=None):
        end = pieces if end is None else end
        need(NEAR, q, end)
        total = term(NEAR, q, slice(begin * PIECE, end * PIECE))
        for p in range(begin, end):
            part = total[:, span(p - begin)]
            if p < pieces - 1:
                send_r[p * 4 + q] = part.astype(jnp.bfloat16)
            elif q < 2:
                send_a[index(NEAR, p), q] = part.astype(jnp.bfloat16)
            else:
                held[NEAR, q - 2, :, span(p)] = part

    def near_rest(q):
        near_some(q, 1)

    def send_raw(q, begin=0, end=None):
        for p in range(begin, pieces - 1 if end is None else end):
            copy_r(p * 4 + q).start()

    def hold(step, q):
        need(step, q, pieces)
        held[step, q - 2] = term(step, q)

    def second(step, p):
        copy_a(step, p, 0).wait_recv()
        total = held[step, 0, :, span(p)] + wide(recv_a.at[index(step, p), 0])
        if step == OWN and p < pieces - 1:
            total = total + raw_in(p, 2)
        send_b[index(step, p)] = total.astype(jnp.bfloat16)
        copy_b(step, p).start()

    def third(step, p):
        copy_a(step, p, 1).wait_recv()
        copy_b(step, p).wait_recv()
        i = index(step, p)
        total = held[step, 1, :, span(p)] + wide(recv_a.at[i, 1]) + wide(recv_b.at[i])
        if step == NEAR:
            send_z[i] = total.astype(jnp.bfloat16)
            copy_z(step, p).start()
            return

        @pl.when(leads(step))
        def _():
            held[step, 1, :, span(p)] = total

        @pl.when(jnp.logical_not(leads(step)))
        def _():
            send_z[i] = total.astype(jnp.bfloat16)
            copy_y(step, p).start()

    def forward(step, p):
        i = index(step, p)

        @pl.when(leads(step))
        def _():
            if relayed and (step, p) == (0, 0):
                pl.semaphore_wait(ready, 1)
            copy_y(step, p).wait_recv()
            total = held[step, 1, :, span(p)] + wide(recv_y.at[i])
            send_z[i] = total.astype(jnp.bfloat16)
            copy_z(step, p).start()

    load_grad(0, 0).wait()
    weigh(0, 0, PIECE)
    divide(act_order[0])
    if relayed:
        pl.semaphore_wait(barrier, len(greet) + jnp.where(leads(0), 1, 0))
        tell_inner(ready)
    else:
        pl.semaphore_wait(barrier, len(greet))
    copy_acts(0, 1).start()
    copy_w(0, 0).start()
    divide(NEAR)
    copy_acts(NEAR, 1).start()
    load_grad(0, 1).wait()
    weigh(0, PIECE, columns)
    for p in range(1, pieces):
        copy_w(0, p).start()
    copy_acts(0, 0).start()
    copy_acts(NEAR, 0).start()
    for j in range(2):
        load_grad(1, j).wait()
    weigh(1, 0, columns)
    for p in range(pieces):
        copy_w(1, p).start()
    for step in act_order[2:]:
        divide(step)
        send_acts(step)

    actions = {
        "F": first, "G": first_rest, "X": send_first, "N": near_some, "M": near_rest, "R": send_raw,
        "H": hold, "S": second, "T": third, "Y": forward,
    }
    for name, *where in plan(fars, pieces):
        actions[name](*where)

    for p in range(pieces):
        i = index(OWN, p)
        width = min(PIECE, columns - p * PIECE)
        total = held[OWN, 1, :, span(p)]
        if p < pieces - 1:
            total = total + raw_in(p, 3)
        copy_a(OWN, p, 1).wait_recv()
        total = total + wide(recv_a.at[i, 1])
        held[OWN, 1, :, span(p)] = total
    for p in range(pieces):
        i = index(OWN, p)
        width = min(PIECE, columns - p * PIECE)
        copy_b(OWN, p).wait_recv()
        total = held[OWN, 1, :, span(p)] + wide(recv_b.at[i])
        for step in range(0, fars, 2):
            copy_z(step, p).wait_recv()
            total = total + wide(recv_z.at[slot(step, p)])
        if p == pieces - 1:
            copy_z(NEAR, p).wait_recv()
            total = total + wide(recv_z.at[slot(NEAR, p)])
        out_ref[:, p * PIECE : p * PIECE + width] = total[:, :width]

    def settle(ref, k):
        remote(ref, ref, (sent.at[k], sent.at[k]), pair_dev).wait_send()

    settle(peer_acts, 0)
    for k, ref in enumerate((mine, send_a, send_b, send_z, send_r)):
        settle(ref, k + 1)


def shards(expert_act, grad_out, slot_token, slot_prob, live_count):
    slots, hidden = expert_act.shape
    tokens = grad_out.shape[0]
    ranks, halves = lax.axis_size("dp"), lax.axis_size("tensor")
    outer = ranks // 4
    rows, columns = hidden // ranks, grad_out.shape[1] // halves
    pieces = pl.cdiv(columns, PIECE)
    count = (outer - 1) * pieces + 1
    raws = 4 * (pieces - 1)
    scaling = 1.0 / math.sqrt(slots * ranks * halves)
    bf16, f32, dma = jnp.bfloat16, jnp.float32, pltpu.SemaphoreType.DMA
    anywhere = pl.BlockSpec(memory_space=pl.ANY)
    total = pl.pallas_call(
        functools.partial(kernel, outer),
        out_shape=jax.ShapeDtypeStruct((rows, columns), f32),
        in_specs=[
            anywhere,
            anywhere,
            pl.BlockSpec(memory_space=pltpu.VMEM),
            pl.BlockSpec(memory_space=pltpu.VMEM),
            pl.BlockSpec(memory_space=pltpu.SMEM),
        ],
        out_specs=pl.BlockSpec(memory_space=pltpu.VMEM),
        scratch_shapes=[
            pltpu.VMEM((outer, 4 * rows, slots), bf16),
            pltpu.VMEM((halves, columns, tokens), bf16),
            pltpu.VMEM((2, outer, 2, rows, slots), bf16),
            pltpu.VMEM((outer, 2, rows, slots), bf16),
            pltpu.VMEM((halves, slots, pieces * PIECE), bf16),
            pltpu.VMEM((halves, slots, pieces * PIECE), bf16),
            pltpu.VMEM((slots, tokens), bf16),
            pltpu.VMEM((slots, LANES), f32),
            pltpu.VMEM((outer, 2, rows, pieces * PIECE), f32),
            pltpu.VMEM((count, 2, rows, PIECE), bf16),
            pltpu.VMEM((count, 2, rows, PIECE), bf16),
            pltpu.VMEM((count, rows, PIECE), bf16),
            pltpu.VMEM((count, rows, PIECE), bf16),
            pltpu.VMEM((count - pieces, rows, PIECE), bf16),
            pltpu.VMEM((count - pieces, rows, PIECE), bf16),
            pltpu.VMEM((count - pieces, rows, PIECE), bf16),
            pltpu.VMEM((raws, rows, PIECE), bf16),
            pltpu.VMEM((raws, rows, PIECE), bf16),
            dma((outer,)),
            dma((2, 2)),
            dma((outer, 2)),
            dma((2, pieces)),
            dma((count, 2)),
            dma((count,)),
            dma(((outer - 2) // 2 * pieces + 1,)),
            dma((count - 1 - pieces,)),
            dma((raws,)),
            dma((6,)),
            pltpu.SemaphoreType.REGULAR,
        ],
        compiler_params=pltpu.CompilerParams(
            collective_id=0, has_side_effects=True, vmem_limit_bytes=53 * 2**20
        ),
    )(
        expert_act.T.reshape(outer, 4 * rows, slots),
        grad_out.T.reshape(halves, columns, tokens),
        slot_token[None, :],
        slot_prob[None, :],
        live_count,
    )
    return total * scaling


def solution(mesh):
    return jax.shard_map(
        shards,
        mesh=mesh,
        in_specs=(
            P(("dp", "tensor"), None),
            P(("dp", "tensor"), None),
            P(("dp", "tensor")),
            P(("dp", "tensor")),
            P(("dp", "tensor")),
        ),
        out_specs=P("dp", "tensor"),
        check_vma=False,
    )
```

```python
import functools
import math

import jax
import jax.numpy as jnp
from jax import lax
from jax.experimental import pallas as pl
from jax.experimental.pallas import tpu as pltpu
from jax.sharding import PartitionSpec as P

MESH = pl.DeviceIdType.MESH
PIECE = 256
LANES = 128


TUNED = (2, 3)
ORDER = (
    "F000", "X000", "N001", "R001", "W0", "G00", "X010", "X020", "W1",
    "F010", "X001", "M0", "X220", "R01", "D", "G01", "X011", "H02",
    "S00", "N1", "S01", "R1", "H03", "X021", "F10", "S02", "F11",
    "H12", "T00", "X100", "H13", "N2", "X110", "N3", "T01", "X120",
    "F30", "H32", "X101", "T02", "R2", "F31", "S10", "X111", "X121",
    "H33", "S11", "S12", "X221", "Y00", "X300", "X310", "T10", "Y01",
    "X320", "T11", "Y02", "X301", "X311", "T12", "S22", "R3", "S30",
    "X321", "T22", "Y10", "S31", "Y11", "Y12", "S32",
)


def plan(fars, pieces):
    if (fars, pieces) == TUNED:
        return [(token[0], *map(int, token[1:])) for token in ORDER]
    near, own, every = fars, fars + 1, range(pieces)
    steps = [("W", 0), ("W", 1), ("D",)]
    steps += [("F", 0, k, p) for k in range(2) for p in every]
    steps += [("X", 0, p, k) for k in range(2) for p in every]
    steps += [(name, q) for q in range(4) for name in "NR"]
    steps += [("X", near, pieces - 1, k) for k in range(2)]
    for j in list(range(fars)) + [near, own]:
        then = j + 1 if j + 1 < fars else own
        if j < near:
            steps += [("F", then, k, p) for k in range(2) for p in every]
            steps += [("H", j, 2), ("H", j, 3)]
        if j == own:
            steps += [("H", j, 2), ("H", j, 3)]
        mine = [pieces - 1] if j == near else every
        steps += [("S", j, p) for p in mine]
        if j < near:
            steps += [("X", then, p, k) for k in range(2) for p in every]
        if j < own:
            steps += [("T", j, p) for p in mine]
        if j < near:
            steps += [("Y", j, p) for p in every]
    return steps


def kernel(
    outer,
    acts_hbm, grad_hbm, token_ref, prob_ref, live_ref, out_ref,
    acts_raw, grad_raw, acts, peer_acts, mine, peer, onehot, weight, held,
    send_a, recv_a, send_b, recv_b, send_z, recv_z, recv_y, send_r, recv_r,
    load_sems, grad_sems, acts_sems, w_sems,
    a_sems, b_sems, z_sems, y_sems, r_sems, sent, ready,
):
    dp = lax.axis_index("dp")
    half = lax.axis_index("tensor")
    core = lax.rem(dp, 2)
    mid = lax.rem(dp // 2, 2)
    own = dp // 4
    my_a = half * (1 - core) + mid * core
    my_b = mid * (1 - core) + half * core
    flip_mid = dp + 2 - 4 * mid
    pair_dev = {"dp": dp + 1 - 2 * core, "tensor": half}
    a_dev = {
        "dp": dp * (1 - core) + flip_mid * core,
        "tensor": (1 - half) * (1 - core) + half * core,
    }
    b_dev = {
        "dp": flip_mid * (1 - core) + dp * core,
        "tensor": half * (1 - core) + (1 - half) * core,
    }
    side = lax.rem(own, 2)
    near = own + 1 - 2 * side
    columns, pieces = out_ref.shape[1], mine.shape[2] // PIECE
    rows, slots = acts.shape[3], acts.shape[4]
    tokens = grad_raw.shape[2]
    fars = outer - 2
    far_total = fars * pieces
    raws = send_r.shape[0]
    spots = ((1 - my_a, 1 - my_b), (1 - my_a, my_b), (my_a, 1 - my_b), (my_a, my_b))

    def far_pair(j):
        pair = lax.rem(own // 2 + 1 + j // 2, outer // 2)
        return pair, jnp.where(pair > own // 2, 1, 0)

    def far(j):
        pair, up = far_pair(j)
        return 2 * pair + (up if j % 2 == 0 else 1 - up)

    def leads(j):
        return side == far_pair(j)[1]

    targets = [far(j) for j in range(fars)] + [near, own]
    NEAR, OWN = fars, fars + 1

    def z_dev(o):
        return {"dp": dp + (o - own) * 4, "tensor": half}

    def remote(src, dst, sems, device):
        return pltpu.make_async_remote_copy(
            src_ref=src, dst_ref=dst, send_sem=sems[0], recv_sem=sems[1],
            device_id=device, device_id_type=MESH,
        )

    grad_order = (1 - half, half)

    def load_grad(i, j):
        g = grad_order[i]
        window = pl.ds(0, PIECE) if j == 0 else pl.ds(PIECE, columns - PIECE)
        return pltpu.make_async_copy(
            grad_hbm.at[g, window], grad_raw.at[g, window], grad_sems.at[i, j]
        )

    def load_acts(step):
        o = targets[step]
        return pltpu.make_async_copy(acts_hbm.at[o], acts_raw.at[o], load_sems.at[step])

    act_order = [0, NEAR] + list(range(1, fars)) + [OWN]
    load_grad(0, 0).start()
    load_acts(act_order[0]).start()
    load_grad(0, 1).start()
    load_acts(act_order[1]).start()
    for j in range(2):
        load_grad(1, j).start()
    for step in act_order[2:]:
        load_acts(step).start()

    barrier = pltpu.get_barrier_semaphore()
    relayed = fars == 2
    greet = [pair_dev, a_dev, b_dev, z_dev(near)]
    if not relayed:
        greet += [z_dev(o) for o in targets[:NEAR]]
    for device in greet:
        pl.semaphore_signal(barrier, inc=1, device_id=device, device_id_type=MESH)

    def tell_inner(semaphore):
        @pl.when(leads(0))
        def _():
            pl.semaphore_signal(
                semaphore, inc=1, device_id=z_dev(far(1)), device_id_type=MESH
            )

    if relayed:
        tell_inner(barrier)

    def turn(row):
        return jnp.broadcast_to(row.astype(jnp.float32), (LANES, slots)).T

    token = turn(token_ref[...])
    lane = lax.broadcasted_iota(jnp.int32, (slots, LANES), 1).astype(jnp.float32)
    for t in range(0, tokens, LANES):
        onehot[:, t : t + LANES] = jnp.where(token - t == lane, 1.0, 0.0).astype(
            onehot.dtype
        )
    live = lax.broadcasted_iota(jnp.int32, (1, slots), 1) < live_ref[0]
    weight[...] = turn(jnp.where(live, prob_ref[...], 0.0))
    if pieces * PIECE > columns:
        ragged = columns // LANES * LANES
        mine[:, :, ragged:] = jnp.zeros(
            (2, slots, pieces * PIECE - ragged), mine.dtype
        )

    def span(p):
        return slice(p * PIECE, (p + 1) * PIECE)

    def copy_w(i, p):
        g = grad_order[i]
        return remote(
            mine.at[g, :, pl.ds(p * PIECE, PIECE)],
            peer.at[g, :, pl.ds(p * PIECE, PIECE)],
            (sent.at[1], w_sems.at[i, p]), pair_dev,
        )

    def copy_acts(step, far_half):
        o, m = targets[step], 1 - mid if far_half else mid
        return remote(
            acts.at[1 - core, o, m], peer_acts.at[o, m],
            (sent.at[0], acts_sems.at[step, far_half]), pair_dev,
        )

    def send_acts(step):
        for far_half in (1, 0):
            copy_acts(step, far_half).start()

    def weigh(i, begin, end):
        g = grad_order[i]
        picked = lax.dot_general(
            onehot[...], grad_raw[g, begin:end], (((1,), (1,)), ((), ())),
            preferred_element_type=jnp.float32,
        )
        for t in range(begin, end, LANES):
            stop = min(t + LANES, end)
            mine[g, :, t:stop] = (
                picked[:, t - begin : stop - begin] * weight[:, : stop - t]
            ).astype(jnp.bfloat16)

    def divide(step):
        o = targets[step]
        load_acts(step).wait()
        for k in range(4):
            acts[k % 2, o, k // 2] = acts_raw[o, k * rows : (k + 1) * rows, :]

    def contract(left, right):
        return jnp.dot(left, right, preferred_element_type=jnp.float32)

    def term(step, q, window=slice(None)):
        o = targets[step]
        a, b = spots[q]
        m = b * (1 - core) + a * core
        column = a * (1 - core) + b * core
        return contract(acts[core, o, m], mine[column, :, window]) + contract(
            peer_acts[o, m], peer[column, :, window]
        )

    def index(step, p):
        return step * pieces + p if step < NEAR else far_total + (0 if step == NEAR else 1 + p)

    def copy_a(step, p, k):
        i = index(step, p)
        return remote(
            send_a.at[i, k], recv_a.at[i, k],
            (sent.at[2], a_sems.at[i, k]), a_dev,
        )

    def copy_b(step, p):
        i = index(step, p)
        return remote(send_b.at[i], recv_b.at[i], (sent.at[3], b_sems.at[i]), b_dev)

    def slot(step, p):
        return step // 2 * pieces + p if step < NEAR else fars // 2 * pieces

    def copy_z(step, p):
        i, j = index(step, p), slot(step, p)
        return remote(
            send_z.at[i], recv_z.at[j], (sent.at[4], z_sems.at[j]),
            z_dev(targets[step]),
        )

    def copy_y(step, p):
        i = index(step, p)
        return remote(
            send_z.at[i], recv_y.at[i], (sent.at[4], y_sems.at[i]), z_dev(near)
        )

    def copy_r(r):
        return remote(
            send_r.at[r], recv_r.at[r], (sent.at[5], r_sems.at[r]), z_dev(near)
        )

    def raw_in(p, q):
        r = p * 4 + q
        copy_r(r).wait_recv()
        return recv_r[r].astype(jnp.float32)

    def wide(ref):
        return ref[...].astype(jnp.float32)

    seen = set()

    def need(step, q, pieces_end):
        wanted = []
        for far_half in (1,) if q == 0 else (1, 0):
            if ("acts", step, far_half) not in seen:
                seen.add(("acts", step, far_half))
                wanted.append(copy_acts(step, far_half))
        for i in range(1 if q == 0 else 2):
            for p in range(pieces_end):
                if (i, p) not in seen:
                    seen.add((i, p))
                    wanted.append(copy_w(i, p))
        for copy in wanted:
            copy.wait_recv()

    def first(step, k, p=None):
        begin, end = (0, pieces) if p is None else (p, p + 1)
        need(step, k, end)
        total = term(step, k, slice(begin * PIECE, end * PIECE))
        for p in range(begin, end):
            part = total[:, span(p - begin)]
            if step == OWN and p < pieces - 1:
                part = part + raw_in(p, k)
            send_a[index(step, p), k] = part.astype(jnp.bfloat16)

    def first_rest(step, k):
        need(step, k, pieces)
        total = term(step, k, slice(PIECE, pieces * PIECE))
        for p in range(1, pieces):
            send_a[index(step, p), k] = total[:, span(p - 1)].astype(jnp.bfloat16)

    def send_first(step, p, k):
        copy_a(step, p, k).start()

    def near_some(q, begin=0, end=None):
        end = pieces if end is None else end
        need(NEAR, q, end)
        total = term(NEAR, q, slice(begin * PIECE, end * PIECE))
        for p in range(begin, end):
            part = total[:, span(p - begin)]
            if p < pieces - 1:
                send_r[p * 4 + q] = part.astype(jnp.bfloat16)
            elif q < 2:
                send_a[index(NEAR, p), q] = part.astype(jnp.bfloat16)
            else:
                held[NEAR, q - 2, :, span(p)] = part

    def near_rest(q):
        near_some(q, 1)

    def send_raw(q, begin=0, end=None):
        for p in range(begin, pieces - 1 if end is None else end):
            copy_r(p * 4 + q).start()

    def hold(step, q):
        need(step, q, pieces)
        held[step, q - 2] = term(step, q)

    def second(step, p):
        copy_a(step, p, 0).wait_recv()
        total = held[step, 0, :, span(p)] + wide(recv_a.at[index(step, p), 0])
        if step == OWN and p < pieces - 1:
            total = total + raw_in(p, 2)
        send_b[index(step, p)] = total.astype(jnp.bfloat16)
        copy_b(step, p).start()

    def third(step, p):
        copy_a(step, p, 1).wait_recv()
        copy_b(step, p).wait_recv()
        i = index(step, p)
        total = held[step, 1, :, span(p)] + wide(recv_a.at[i, 1]) + wide(recv_b.at[i])
        if step == NEAR:
            send_z[i] = total.astype(jnp.bfloat16)
            copy_z(step, p).start()
            return

        @pl.when(leads(step))
        def _():
            held[step, 1, :, span(p)] = total

        @pl.when(jnp.logical_not(leads(step)))
        def _():
            send_z[i] = total.astype(jnp.bfloat16)
            copy_y(step, p).start()

    def forward(step, p):
        i = index(step, p)

        @pl.when(leads(step))
        def _():
            if relayed and (step, p) == (0, 0):
                pl.semaphore_wait(ready, 1)
            copy_y(step, p).wait_recv()
            total = held[step, 1, :, span(p)] + wide(recv_y.at[i])
            send_z[i] = total.astype(jnp.bfloat16)
            copy_z(step, p).start()

    load_grad(0, 0).wait()
    weigh(0, 0, PIECE)
    divide(act_order[0])
    if relayed:
        pl.semaphore_wait(barrier, len(greet) + jnp.where(leads(0), 1, 0))
        tell_inner(ready)
    else:
        pl.semaphore_wait(barrier, len(greet))
    copy_acts(0, 1).start()
    copy_w(0, 0).start()
    divide(NEAR)
    copy_acts(NEAR, 1).start()
    load_grad(0, 1).wait()
    weigh(0, PIECE, columns)
    for p in range(1, pieces):
        copy_w(0, p).start()
    copy_acts(0, 0).start()
    copy_acts(NEAR, 0).start()

    def weigh_mine(part):
        begin, end = (0, 1) if part == 0 else (1, pieces)
        load_grad(1, part).wait()
        weigh(1, begin * PIECE, min(end * PIECE, columns))
        for p in range(begin, end):
            copy_w(1, p).start()

    def divide_rest():
        for step in act_order[2:]:
            divide(step)
            send_acts(step)

    actions = {
        "F": first, "G": first_rest, "X": send_first, "N": near_some, "M": near_rest, "R": send_raw,
        "W": weigh_mine, "D": divide_rest, "H": hold, "S": second, "T": third, "Y": forward,
    }
    for name, *where in plan(fars, pieces):
        actions[name](*where)

    for p in range(pieces):
        i = index(OWN, p)
        width = min(PIECE, columns - p * PIECE)
        total = held[OWN, 1, :, span(p)]
        if p < pieces - 1:
            total = total + raw_in(p, 3)
        copy_a(OWN, p, 1).wait_recv()
        total = total + wide(recv_a.at[i, 1])
        held[OWN, 1, :, span(p)] = total
    for p in range(pieces):
        i = index(OWN, p)
        width = min(PIECE, columns - p * PIECE)
        copy_b(OWN, p).wait_recv()
        total = held[OWN, 1, :, span(p)] + wide(recv_b.at[i])
        for step in range(0, fars, 2):
            copy_z(step, p).wait_recv()
            total = total + wide(recv_z.at[slot(step, p)])
        if p == pieces - 1:
            copy_z(NEAR, p).wait_recv()
            total = total + wide(recv_z.at[slot(NEAR, p)])
        out_ref[:, p * PIECE : p * PIECE + width] = total[:, :width]

    def settle(ref, k):
        remote(ref, ref, (sent.at[k], sent.at[k]), pair_dev).wait_send()

    settle(peer_acts, 0)
    for k, ref in enumerate((mine, send_a, send_b, send_z, send_r)):
        settle(ref, k + 1)


def shards(expert_act, grad_out, slot_token, slot_prob, live_count):
    slots, hidden = expert_act.shape
    tokens = grad_out.shape[0]
    ranks, halves = lax.axis_size("dp"), lax.axis_size("tensor")
    outer = ranks // 4
    rows, columns = hidden // ranks, grad_out.shape[1] // halves
    pieces = pl.cdiv(columns, PIECE)
    count = (outer - 1) * pieces + 1
    raws = 4 * (pieces - 1)
    scaling = 1.0 / math.sqrt(slots * ranks * halves)
    bf16, f32, dma = jnp.bfloat16, jnp.float32, pltpu.SemaphoreType.DMA
    anywhere = pl.BlockSpec(memory_space=pl.ANY)
    total = pl.pallas_call(
        functools.partial(kernel, outer),
        out_shape=jax.ShapeDtypeStruct((rows, columns), f32),
        in_specs=[
            anywhere,
            anywhere,
            pl.BlockSpec(memory_space=pltpu.VMEM),
            pl.BlockSpec(memory_space=pltpu.VMEM),
            pl.BlockSpec(memory_space=pltpu.SMEM),
        ],
        out_specs=pl.BlockSpec(memory_space=pltpu.VMEM),
        scratch_shapes=[
            pltpu.VMEM((outer, 4 * rows, slots), bf16),
            pltpu.VMEM((halves, columns, tokens), bf16),
            pltpu.VMEM((2, outer, 2, rows, slots), bf16),
            pltpu.VMEM((outer, 2, rows, slots), bf16),
            pltpu.VMEM((halves, slots, pieces * PIECE), bf16),
            pltpu.VMEM((halves, slots, pieces * PIECE), bf16),
            pltpu.VMEM((slots, tokens), bf16),
            pltpu.VMEM((slots, LANES), f32),
            pltpu.VMEM((outer, 2, rows, pieces * PIECE), f32),
            pltpu.VMEM((count, 2, rows, PIECE), bf16),
            pltpu.VMEM((count, 2, rows, PIECE), bf16),
            pltpu.VMEM((count, rows, PIECE), bf16),
            pltpu.VMEM((count, rows, PIECE), bf16),
            pltpu.VMEM((count - pieces, rows, PIECE), bf16),
            pltpu.VMEM((count - pieces, rows, PIECE), bf16),
            pltpu.VMEM((count - pieces, rows, PIECE), bf16),
            pltpu.VMEM((raws, rows, PIECE), bf16),
            pltpu.VMEM((raws, rows, PIECE), bf16),
            dma((outer,)),
            dma((2, 2)),
            dma((outer, 2)),
            dma((2, pieces)),
            dma((count, 2)),
            dma((count,)),
            dma(((outer - 2) // 2 * pieces + 1,)),
            dma((count - 1 - pieces,)),
            dma((raws,)),
            dma((6,)),
            pltpu.SemaphoreType.REGULAR,
        ],
        compiler_params=pltpu.CompilerParams(
            collective_id=0, has_side_effects=True, vmem_limit_bytes=53 * 2**20
        ),
    )(
        expert_act.T.reshape(outer, 4 * rows, slots),
        grad_out.T.reshape(halves, columns, tokens),
        slot_token[None, :],
        slot_prob[None, :],
        live_count,
    )
    return total * scaling


def solution(mesh):
    return jax.shard_map(
        shards,
        mesh=mesh,
        in_specs=(
            P(("dp", "tensor"), None),
            P(("dp", "tensor"), None),
            P(("dp", "tensor")),
            P(("dp", "tensor")),
            P(("dp", "tensor")),
        ),
        out_specs=P("dp", "tensor"),
        check_vma=False,
    )
```
